32 devices in a mesh: slides: 2 (over y), seq: 4 (over z), sub: 4 (over x, core).
Axes of the slice: x: 2, y: 2, z: 4, core: 2. Of those that a mesh axis runs over, the one named last changes fastest.
Arguments:
- q_heads: bfloat16 [8192, 768], P(('slides', 'seq'), 'sub'), parts along dimension 0, may hold values from -8 to 8
- k_heads: bfloat16 [8192, 768], P(('slides', 'seq'), 'sub'), parts along dimension 0, may hold values from -8 to 8
- v_heads: bfloat16 [8192, 768], P(('slides', 'seq'), 'sub'), parts along dimension 0, may hold values from -6 to 6
- w_out: bfloat16 [768, 768], replicated, may hold values from -0.21875 to 0.21875
- offsets: int32 [2, 16], replicated, may hold values from 0 to 15, as said below
- valid: int32 [2], P('slides'), parts along dimension 0, may hold values from 3073 to 4096
Outputs:
- mixed: bfloat16 [8192, 768], P(('slides', 'seq'), 'sub'), parts along dimension 0
The draws below stay inside these ranges and needn't reach their ends.
There are 2 independent parts, one for each index of `slides`. The reference program is written for one: setup_inputs(seed, part) draws one part's arguments, and reference() takes and returns one part's arrays. A program takes and returns all parts, laid end to end along the dimension named above; an argument that names none is the same for every part. Nothing has to cross between parts.
Inputs may be any that keep to these rules, and one draw needn't show every extreme that they name: `offsets`: row 0 lies below 4, row 1 below 16. Tiles at positions valid[0] and beyond are padding.
All inputs are finite; a program needn't handle non-finite values.
Results may differ from the reference program's by a relative error of at most 0.012.
Values may be sent and summed in bfloat16 or wider, within the bound.
A program may use at most 64 MiB of HBM per device.

```python
import jax
import jax.numpy as jnp
from jax import lax

D = 768
H = 16
HS = 48
TOK_DEV = 1024
GROUP = 4
R1 = 4
R2 = 16
TOKENS = 4096


def paired_fields(key):
    first_key = jax.random.fold_in(key, 101)
    second_key = jax.random.fold_in(key, 202)
    query = jnp.clip(2.0 * jax.random.normal(first_key, (TOKENS, D), jnp.float32), -8.0, 8.0)
    key_out = jnp.clip(2.0 * jax.random.normal(second_key, (TOKENS, D), jnp.float32), -8.0, 8.0)
    return (query, key_out)


def draw_q_heads(key, part):
    return paired_fields(key)[0].astype(jnp.bfloat16)


def draw_k_heads(key, part):
    return paired_fields(key)[1].astype(jnp.bfloat16)


def draw_offsets(key, part):
    middle = jax.random.randint(jax.random.fold_in(key, 7), (H,), 0, R1).astype(jnp.int32)
    widest = jax.random.randint(jax.random.fold_in(key, 8), (H,), 0, R2).astype(jnp.int32)
    low_head = jax.random.randint(jax.random.fold_in(key, 9), (), 0, H)
    high_head = jax.random.randint(jax.random.fold_in(key, 10), (), 0, H)
    top_head = jax.random.randint(jax.random.fold_in(key, 11), (), 0, H)
    middle = middle.at[low_head].set(0)
    middle = middle.at[(low_head + 1 + top_head % (H - 1)) % H].set(R1 - 1)
    widest = widest.at[high_head].set(R2 - 1)
    return jnp.stack([middle, widest], axis=0).astype(jnp.int32)


def shard_levels(own_key, extent, shards, least, top_value):
    level, own = 1.0, jax.random.fold_in(own_key, 6)
    for axis_at, shards_of in shards:
        steps = jnp.exp(jax.random.uniform(jax.random.fold_in(own, axis_at), (shards_of,), jnp.float32, least / len(shards), top_value / len(shards)))
        level = level * jnp.repeat(steps, extent[axis_at] // shards_of).reshape([-1 if axis == axis_at else 1 for axis in range(len(extent))])
    return level


def noise(key, dims, width, most, cuts=(), kind=jnp.bfloat16):
    values = width * jax.random.normal(key, dims, jnp.float32)
    if cuts:
        values = values * shard_levels(key, dims, cuts, -0.22, 0.18)
    return jnp.clip(values, -most, most).astype(kind)


def setup_inputs(seed: int = 0, part: int = 0) -> dict:
    keys = jax.random.split(jax.random.key(seed), 7)
    own_keys = jax.random.split(jax.random.fold_in(keys[6], part), 7)
    q_heads = draw_q_heads(jax.random.fold_in(jax.random.fold_in(keys[6], part), 71), part)
    k_heads = draw_k_heads(jax.random.fold_in(jax.random.fold_in(keys[6], part), 71), part)
    v_heads = noise(own_keys[2], (TOKENS, D), 1.0, 6.0, ((0, 4), (1, 4)))
    w_out = noise(keys[3], (D, D), D ** -0.5, 0.21875)
    offsets = draw_offsets(jax.random.fold_in(keys[6], 71), part)
    valid = jax.random.randint(own_keys[5], (1,), TOKENS - TOK_DEV + 1, TOKENS + 1).astype(jnp.int32)
    return dict(q_heads=q_heads, k_heads=k_heads, v_heads=v_heads, w_out=w_out, offsets=offsets, valid=valid)


NEG_FILL = -1.0e30


def pick_rows(source, stride, chosen):
    grouped = source.reshape(source.shape[0] // stride, stride, source.shape[1], source.shape[2])
    onehot = jnp.arange(stride, dtype=jnp.int32)[:, None] == chosen[None, :]
    return jnp.sum(jnp.where(onehot[None, :, :, None], grouped, jnp.zeros((), source.dtype)), axis=1)


def spread_back(maxima, totals, numer, stride, chosen):
    onehot = (jnp.arange(stride, dtype=jnp.int32)[:, None] == chosen[None, :])[None]
    count = maxima.shape[0] * stride
    full_max = jnp.where(onehot, maxima[:, None, :], NEG_FILL).reshape(count, maxima.shape[1])
    full_tot = jnp.where(onehot, totals[:, None, :], 0.0).reshape(count, maxima.shape[1])
    full_num = jnp.where(onehot[..., None], numer[:, None, :, :], 0.0).reshape(count, numer.shape[1], numer.shape[2])
    return full_max, full_tot, full_num


def one_branch(query, key_in, value, seg_len, stride, chosen, limit):
    total_rows = query.shape[0]
    heads = query.shape[1]
    q_sel = pick_rows(query, stride, chosen)
    k_sel = pick_rows(key_in, stride, chosen)
    v_sel = pick_rows(value, stride, chosen)
    per_seg = seg_len // stride
    n_segs = total_rows // seg_len
    positions = jnp.arange(total_rows // stride, dtype=jnp.int32)[:, None] * stride + chosen[None, :]
    live = positions < limit

    def arrange(block):
        moved = jnp.moveaxis(block, 1, 0)
        return moved.reshape((heads * n_segs, per_seg) + moved.shape[2:])

    def attend(items):
        q_blk, k_blk, v_blk, l_blk = items
        scores = jnp.dot(q_blk, k_blk.T, preferred_element_type=jnp.float32) * (HS ** -0.5)
        scores = jnp.where(l_blk[None, :], scores, NEG_FILL)
        peak = jnp.max(scores, axis=1)
        probs = jnp.exp(scores - peak[:, None])
        mass = jnp.sum(probs, axis=1)
        numer = jnp.dot(probs.astype(jnp.bfloat16), v_blk, preferred_element_type=jnp.float32)
        return peak, mass, numer

    peak, mass, numer = lax.map(attend, (arrange(q_sel), arrange(k_sel), arrange(v_sel), arrange(live)))
    peak = peak.reshape(heads, total_rows // stride).T
    mass = mass.reshape(heads, total_rows // stride).T
    numer = jnp.moveaxis(numer.reshape(heads, total_rows // stride, HS), 0, 1)
    return spread_back(peak, mass, numer, stride, chosen)


def reference(q_heads, k_heads, v_heads, w_out, offsets, valid):
    total_rows = q_heads.shape[0]
    query = q_heads.reshape(total_rows, H, HS)
    key_in = k_heads.reshape(total_rows, H, HS)
    value = v_heads.reshape(total_rows, H, HS)
    limit = valid[0]
    zero_offs = jnp.zeros((H,), jnp.int32)
    branches = [
        one_branch(query, key_in, value, TOK_DEV, 1, zero_offs, limit),
        one_branch(query, key_in, value, GROUP * TOK_DEV, R1, offsets[0], limit),
        one_branch(query, key_in, value, TOKENS, R2, offsets[1], limit),
    ]
    top = jnp.maximum(jnp.maximum(branches[0][0], branches[1][0]), branches[2][0])
    denom = jnp.zeros_like(top)
    numer = jnp.zeros_like(branches[0][2])
    for peak, mass, partial_num in branches:
        weight = jnp.exp(peak - top)
        denom = denom + weight * mass
        numer = numer + weight[..., None] * partial_num
    attn = (numer / denom[..., None]).reshape(total_rows, D).astype(jnp.bfloat16)
    projected = jnp.dot(attn, w_out, preferred_element_type=jnp.float32)
    keep = jnp.arange(total_rows, dtype=jnp.int32) < limit
    return jnp.where(keep[:, None], projected, 0.0).astype(jnp.bfloat16)
```

```python
import functools

import jax
import jax.numpy as jnp
from jax import lax
from jax.experimental import pallas as pl
from jax.experimental.pallas import tpu as pltpu
from jax.sharding import PartitionSpec as P

HS = 48
GROUP = 4
R1 = 4
R2 = 16
LANES = 128
HALF = 64
MASKED = -1e30
MESH = pl.DeviceIdType.MESH
EXP_SCALE = HS ** (-0.5) * 1.4426950408889634


def pick(masks, parts):
    out = parts[-1]
    for mask, part in zip(masks[:-1], parts[:-1]):
        out = jnp.where(mask, part, out)
    return out


def kernel(
    n_seq, n_sub, heads,
    q_ref, k_ref, v_ref, w_ref, off_ref, valid_ref, o_ref,
    sq, sk, sv, qp, kx, vx, qm, qw, wide, mid, wk, wv, mk, mv,
    st_m, st_l, st_a, xg, wl, wr, so,
    wide_send, wide_recv, mid_send, mid_recv, x_send, x_recv,
):
    rows = q_ref.shape[0]
    cols = heads * HS
    phase = rows // R1
    strip = rows // R2
    subs = R2 // R1
    half_rows = phase // 2
    seq = lax.axis_index("seq")
    sub = lax.axis_index("sub")
    pos = lax.rem(seq, GROUP)
    group0 = seq - pos
    limit = valid_ref[0]
    has_left = pos > 0
    has_right = pos < GROUP - 1
    bits = [1 << b for b in reversed(range(n_sub.bit_length() - 1))]

    barrier = pltpu.get_barrier_semaphore()
    for step in range(1, n_seq):
        pl.semaphore_signal(
            barrier, inc=1, device_id={"seq": lax.rem(seq + step, n_seq)}, device_id_type=MESH
        )
    for bit in bits:
        pl.semaphore_signal(barrier, inc=1, device_id={"sub": sub ^ bit}, device_id_type=MESH)

    lane = lax.broadcasted_iota(jnp.int32, (1, LANES), 1)
    low = lane < HALF

    def off_lanes(which, first_head, base, tile):
        at = lane + tile * LANES - base
        out = jnp.zeros((1, LANES), jnp.int32)
        for h in range(heads):
            here = ((at >= h * HS) & (at < (h + 1) * HS)) | (at == cols + h)
            out = jnp.where(here, off_ref[which, first_head + h], out)
        return out

    def head_mask(h, base, tiles=2):
        at = lax.broadcasted_iota(jnp.int32, (1, tiles * LANES), 1) - base
        here = (at >= h * HS) & (at < (h + 1) * HS)
        if base == 0:
            here = here | (at == cols + h)
        return here

    mine = sub * heads
    left_off = [[off_lanes(b, mine, 0, t) for t in range(2)] for b in range(2)]
    right_off = [[off_lanes(b, mine, HALF, t) for t in range(2)] for b in range(2)]
    kv_off = [
        [left_off[b][0], jnp.where(low, left_off[b][1], right_off[b][0]), right_off[b][1]]
        for b in range(2)
    ]

    for dst, src in ((sq, q_ref), (sk, k_ref), (sv, v_ref)):
        dst[0, :, :] = src[:, :LANES].astype(jnp.float32)
        dst[1, :, :HALF] = src[:, LANES:].astype(jnp.float32)

    row64 = lax.broadcasted_iota(jnp.int32, (strip, LANES), 0) * R2
    block0 = seq * rows
    wide_kv = [None] * 3
    wide_q = [None] * 2
    for a in range(subs):
        mid_kv = [None] * 3
        mid_q = [None] * 2
        for m in range(R1):
            j = a * R1 + m
            at = pl.ds(j, strip, stride=R2)
            to = pl.ds(m * phase + a * strip, strip)
            k0, k1 = sk[0, at, :], sk[1, at, :]
            v0, v1 = sv[0, at, :], sv[1, at, :]
            q0, q1 = sq[0, at, :], sq[1, at, :]
            v0 = pltpu.roll(v0, HALF, 1)
            v1 = pltpu.roll(v1, HALF, 1)
            q1 = jnp.where(low, q1, 1.0)
            t1 = jnp.where(low, k1, v0)
            t2 = jnp.where(low, v0, v1)
            dead = jnp.where(block0 + row64 + j < limit, 0.0, MASKED)
            qp[to, :LANES] = q0.astype(jnp.bfloat16)
            qp[to, LANES:] = q1.astype(jnp.bfloat16)
            kx[to, :LANES] = k0.astype(jnp.bfloat16)
            kx[to, LANES:] = jnp.where(low, k1, dead).astype(jnp.bfloat16)
            vx[to, :LANES] = jnp.where(low, 1.0, v0).astype(jnp.bfloat16)
            vx[to, LANES:] = t2.astype(jnp.bfloat16)
            for i, tile in enumerate((k0, t1, t2)):
                mid_kv[i] = tile if m == 0 else jnp.where(kv_off[0][i] == m, tile, mid_kv[i])
                wide_kv[i] = tile if j == 0 else jnp.where(kv_off[1][i] == j, tile, wide_kv[i])
            for i, tile in enumerate((q0, q1)):
                mid_q[i] = tile if m == 0 else jnp.where(left_off[0][i] == m, tile, mid_q[i])
                wide_q[i] = tile if j == 0 else jnp.where(left_off[1][i] == j, tile, wide_q[i])
        to = pl.ds((a % 2) * strip, strip)
        for i in range(3):
            mid[pos, a // 2, to, i * LANES:(i + 1) * LANES] = mid_kv[i].astype(jnp.bfloat16)
        for i in range(2):
            qm[pl.ds(a * strip, strip), i * LANES:(i + 1) * LANES] = mid_q[i].astype(jnp.bfloat16)
    for i in range(3):
        wide[seq, :, i * LANES:(i + 1) * LANES] = wide_kv[i].astype(jnp.bfloat16)
    for i in range(2):
        qw[:, i * LANES:(i + 1) * LANES] = wide_q[i].astype(jnp.bfloat16)

    pl.semaphore_wait(barrier, n_seq - 1 + len(bits))

    def wide_copy(origin, step):
        return pltpu.make_async_remote_copy(
            src_ref=wide.at[origin], dst_ref=wide.at[origin],
            send_sem=wide_send.at[step], recv_sem=wide_recv.at[step],
            device_id={"seq": lax.rem(seq + step, n_seq)}, device_id_type=MESH,
        )

    for step in range(1, n_seq):
        wide_copy(seq, step).start()

    def mid_copy(origin, chunk, rightward):
        way = 0 if rightward else 1
        target = seq + 1 if rightward else seq - 1
        return pltpu.make_async_remote_copy(
            src_ref=mid.at[origin, chunk], dst_ref=mid.at[origin, chunk],
            send_sem=mid_send.at[way, origin, chunk], recv_sem=mid_recv.at[origin, chunk],
            device_id={"seq": target}, device_id_type=MESH,
        )

    for chunk in range(2):
        @pl.when(has_right)
        def _():
            mid_copy(pos, chunk, True).start()

        @pl.when(has_left)
        def _():
            mid_copy(pos, chunk, False).start()

    def relay(dist, chunk):
        @pl.when(pos - dist >= 0)
        def _():
            mid_copy(pos - dist, chunk, True).wait_recv()

            @pl.when(has_right)
            def _():
                mid_copy(pos - dist, chunk, True).start()

        @pl.when(pos + dist < GROUP)
        def _():
            mid_copy(pos + dist, chunk, False).wait_recv()

            @pl.when(has_left)
            def _():
                mid_copy(pos + dist, chunk, False).start()

    for d in range(n_sub):
        wl[d, pl.ds(cols, HALF), :] = jnp.zeros((HALF, cols), jnp.bfloat16)
        wr[d, pl.ds(0, HALF), :] = jnp.zeros((HALF, cols), jnp.bfloat16)
    for s in range(n_sub):
        @pl.when(sub == s)
        def _():
            for d in range(n_sub):
                part = w_ref[d * cols:(d + 1) * cols, s * cols:(s + 1) * cols]
                wl[d, pl.ds(0, cols), :] = part
                wr[d, pl.ds(HALF, cols), :] = part

    contract_last = (((1,), (1,)), ((), ()))

    def attend(q_blk, keys, values, h, before=None):
        masked_q = jnp.where(head_mask(h, 0), q_blk.astype(jnp.float32), 0.0).astype(jnp.bfloat16)
        scores = lax.dot_general(masked_q, keys, contract_last, preferred_element_type=jnp.float32)
        peak = jnp.max(scores, axis=1, keepdims=True)
        if before is not None:
            peak = jnp.maximum(peak, before)
        probs = jnp.exp2((scores - peak) * EXP_SCALE).astype(jnp.bfloat16)
        return peak, jnp.dot(probs, values, preferred_element_type=jnp.float32)

    def near_step(m, carry):
        at = pl.ds(pl.multiple_of(m * phase, phase), phase)
        q_blk = qp[at, :]
        acc = top = mass = None
        for h in range(heads):
            peak, out = attend(q_blk, kx[...], vx[...], h)
            here = head_mask(h, HALF)
            total = out[:, 0:1]
            shape = out.shape
            if h == 0:
                acc, top, mass = out, jnp.broadcast_to(peak, shape), jnp.broadcast_to(total, shape)
            else:
                acc = jnp.where(here, out, acc)
                top = jnp.where(here, peak, top)
                mass = jnp.where(here, total, mass)
        st_a[at, :] = acc
        st_m[at, :] = top
        st_l[at, :] = mass

        @pl.when(m == 2)
        def _():
            relay(1, 0)

        return carry

    lax.fori_loop(0, R1, near_step, 0)
    relay(1, 1)

    def merge(q_blk, keys, values, top, mass, acc):
        for h in range(heads):
            here = head_mask(h, HALF)
            before = jnp.max(jnp.where(here, top, -3e38), axis=1, keepdims=True)
            peak, out = attend(q_blk, keys, values, h, before)
            fade = jnp.exp2((before - peak) * EXP_SCALE)
            total = out[:, 0:1]
            acc = jnp.where(here, acc * fade + out, acc)
            mass = jnp.where(here, mass * fade + total, mass)
            top = jnp.where(here, peak, top)
        return top, mass, acc

    r_off = [jnp.concatenate(right_off[b], axis=1) for b in range(2)]
    wide_lane_off = left_off[1][1]
    for step in range(1, n_seq):
        wide_copy(lax.rem(seq + n_seq - step, n_seq), step).wait_recv()
    for o in range(n_seq):
        at = pl.ds(o * strip, strip)
        tile1 = wide[o, :, LANES:2 * LANES].astype(jnp.float32)
        dead = jnp.where(o * rows + row64 + wide_lane_off < limit, 0.0, MASKED)
        wk[at, :LANES] = wide[o, :, :LANES]
        wk[at, LANES:] = jnp.where(low, tile1, dead).astype(jnp.bfloat16)
        wv[at, :LANES] = jnp.where(low, 1.0, tile1).astype(jnp.bfloat16)
        wv[at, LANES:] = wide[o, :, 2 * LANES:]

    def strip_at(j):
        return pl.ds((j % R1) * phase + (j // R1) * strip, strip)

    wide_masks = [r_off[1] == j for j in range(R2)]
    state = [pick(wide_masks, [ref[strip_at(j), :] for j in range(R2)]) for ref in (st_m, st_l, st_a)]
    state = merge(qw[...], wk[...], wv[...], *state)
    for ref, new in zip((st_m, st_l, st_a), state):
        for j in range(R2):
            ref[strip_at(j), :] = jnp.where(wide_masks[j], new, ref[strip_at(j), :])

    def pack(slab, value):
        top_half, bot = value[:half_rows], value[half_rows:]
        moved = pltpu.roll(top_half, LANES + HALF, 1)
        xg[sub, slab, :, :LANES] = moved[:, :LANES].astype(jnp.bfloat16)
        xg[sub, slab, :, LANES:2 * LANES] = jnp.where(
            low, moved[:, LANES:], bot[:, :LANES]
        ).astype(jnp.bfloat16)
        xg[sub, slab, :, 2 * LANES:] = bot[:, LANES:].astype(jnp.bfloat16)

    def x_copy(at_bit, held, slab):
        bit = bits[at_bit]
        block = sub ^ held
        return pltpu.make_async_remote_copy(
            src_ref=xg.at[block, slab], dst_ref=xg.at[block, slab],
            send_sem=x_send.at[at_bit, held, slab], recv_sem=x_recv.at[held ^ bit, slab],
            device_id={"sub": sub ^ bit}, device_id_type=MESH,
        )

    def x_plan():
        held, plan = [0], []
        for at_bit, bit in enumerate(bits):
            plan += [(at_bit, x) for x in held]
            held = held + [x ^ bit for x in held]
        return plan

    def x_start(slab):
        for at_bit, x in x_plan():
            if x == 0:
                x_copy(at_bit, x, slab).start()

    def x_recv_wait(block, slab):
        pltpu.make_async_remote_copy(
            src_ref=xg.at[sub ^ block, slab], dst_ref=xg.at[sub ^ block, slab],
            send_sem=x_send.at[0, 0, slab], recv_sem=x_recv.at[block, slab],
            device_id={"sub": sub ^ block}, device_id_type=MESH,
        ).wait_recv()

    def x_forward(slab):
        waited = set()
        for at_bit, x in x_plan():
            if x:
                if x not in waited:
                    waited.add(x)
                    x_recv_wait(x, slab)
                x_copy(at_bit, x, slab).start()
        return waited

    def x_finish(slab, waited):
        for x in range(1, n_sub):
            if x not in waited:
                x_recv_wait(x, slab)

    mid_masks = [r_off[0] == m for m in range(R1)]
    for slab in range(1, R1):
        parts = []
        for m in range(R1):
            at = pl.ds(m * phase, phase)
            parts.append(st_a[at, :] / st_l[at, :])
        pack(slab, pick([mid_masks[(m - slab) % R1] for m in range(R1)], parts))
        x_start(slab)

    for chunk in range(2):
        relay(2, chunk)
    for chunk in range(2):
        relay(3, chunk)

    mid_lane_off = left_off[0][1]
    pair_row = lax.broadcasted_iota(jnp.int32, (half_rows, LANES), 0)
    pair_row = (pair_row % strip) * R2 + (pair_row // strip) * R1
    for o in range(GROUP):
        for chunk in range(2):
            at = pl.ds(o * phase + chunk * half_rows, half_rows)
            tile1 = mid[o, chunk, :, LANES:2 * LANES].astype(jnp.float32)
            place = (group0 + o) * rows + pair_row + (chunk * 2 * R1 + mid_lane_off)
            dead = jnp.where(place < limit, 0.0, MASKED)
            mk[at, :LANES] = mid[o, chunk, :, :LANES]
            mk[at, LANES:] = jnp.where(low, tile1, dead).astype(jnp.bfloat16)
            mv[at, :LANES] = jnp.where(low, 1.0, tile1).astype(jnp.bfloat16)
            mv[at, LANES:] = mid[o, chunk, :, 2 * LANES:]
    state = [
        pick(mid_masks, [ref[pl.ds(m * phase, phase), :] for m in range(R1)])
        for ref in (st_m, st_l, st_a)
    ]
    state = merge(qm[...], mk[...], mv[...], *state)
    pack(0, state[2] / state[1])
    x_start(0)

    done = {}
    for slab in (1, 2, 3, 0):
        done[slab] = x_forward(slab)
    for slab in (1, 2, 3, 0):
        x_finish(slab, done[slab])

    outs = [[None, None] for _ in range(R1)]
    for d in range(n_sub):
        offs = [
            jnp.concatenate([off_lanes(0, d * heads, base, t) for t in range(2)], axis=1)
            for base in (0, HALF)
        ]
        for half in range(2):
            take = slice(half * LANES, half * LANES + 2 * LANES)
            slabs = [xg[d, i, :, take].astype(jnp.float32) for i in range(R1)]
            weights = (wl, wr)[half][d]
            for m in range(R1):
                masks = [offs[half] == (m - i) % R1 for i in range(R1)]
                term = jnp.dot(
                    pick(masks, slabs).astype(jnp.bfloat16), weights,
                    preferred_element_type=jnp.float32,
                )
                outs[m][half] = term if d == 0 else outs[m][half] + term
    for m in range(R1):
        for half in range(2):
            for s in range(2):
                a = half * 2 + s
                res = outs[m][half][s * strip:(s + 1) * strip]
                at = pl.ds(a * R1 + m, strip, stride=R2)
                so[0, at, :] = res[:, :LANES]
                so[1, at, :HALF] = res[:, LANES:]
    keep = block0 + lax.broadcasted_iota(jnp.int32, (rows, 1), 0) < limit
    o_ref[:, :LANES] = jnp.where(keep, so[0, :, :], 0.0).astype(jnp.bfloat16)
    o_ref[:, LANES:] = jnp.where(keep, so[1, :, :HALF], 0.0).astype(jnp.bfloat16)

    for step in range(1, n_seq):
        wide_copy(seq, step).wait_send()
    for chunk in range(2):
        for o in range(GROUP):
            @pl.when(has_right & (pos >= o))
            def _():
                mid_copy(o, chunk, True).wait_send()

            @pl.when(has_left & (pos <= o))
            def _():
                mid_copy(o, chunk, False).wait_send()
    for slab in range(R1):
        for at_bit, x in x_plan():
            x_copy(at_bit, x, slab).wait_send()


def local(n_seq, n_sub, q_heads, k_heads, v_heads, w_out, offsets, valid):
    rows, cols = q_heads.shape
    heads = cols // HS
    phase, strip = rows // R1, rows // R2
    bf, f32 = jnp.bfloat16, jnp.float32
    n_bits = n_sub.bit_length() - 1
    assert cols == LANES + HALF and n_sub == 1 << n_bits
    vmem = pl.BlockSpec(memory_space=pltpu.VMEM)
    smem = pl.BlockSpec(memory_space=pltpu.SMEM)
    wide_all = n_seq * strip
    return pl.pallas_call(
        functools.partial(kernel, n_seq, n_sub, heads),
        out_shape=jax.ShapeDtypeStruct((rows, cols), bf),
        in_specs=[vmem] * 4 + [smem] * 2,
        out_specs=vmem,
        scratch_shapes=[
            pltpu.VMEM((2, rows, LANES), f32),
            pltpu.VMEM((2, rows, LANES), f32),
            pltpu.VMEM((2, rows, LANES), f32),
            pltpu.VMEM((rows, 2 * LANES), bf),
            pltpu.VMEM((rows, 2 * LANES), bf),
            pltpu.VMEM((rows, 2 * LANES), bf),
            pltpu.VMEM((phase, 2 * LANES), bf),
            pltpu.VMEM((strip, 2 * LANES), bf),
            pltpu.VMEM((n_seq, strip, 3 * LANES), bf),
            pltpu.VMEM((GROUP, 2, phase // 2, 3 * LANES), bf),
            pltpu.VMEM((wide_all, 2 * LANES), bf),
            pltpu.VMEM((wide_all, 2 * LANES), bf),
            pltpu.VMEM((GROUP * phase, 2 * LANES), bf),
            pltpu.VMEM((GROUP * phase, 2 * LANES), bf),
            pltpu.VMEM((rows, 2 * LANES), f32),
            pltpu.VMEM((rows, 2 * LANES), f32),
            pltpu.VMEM((rows, 2 * LANES), f32),
            pltpu.VMEM((n_sub, R1, phase // 2, 3 * LANES), bf),
            pltpu.VMEM((n_sub, 2 * LANES, cols), bf),
            pltpu.VMEM((n_sub, 2 * LANES, cols), bf),
            pltpu.VMEM((2, rows, LANES), f32),
            pltpu.SemaphoreType.DMA((n_seq,)),
            pltpu.SemaphoreType.DMA((n_seq,)),
            pltpu.SemaphoreType.DMA((2, GROUP, 2)),
            pltpu.SemaphoreType.DMA((GROUP, 2)),
            pltpu.SemaphoreType.DMA((n_bits, n_sub, R1)),
            pltpu.SemaphoreType.DMA((n_sub, R1)),
        ],
        compiler_params=pltpu.CompilerParams(
            collective_id=0, has_side_effects=True, vmem_limit_bytes=56 * 1024 * 1024
        ),
    )(q_heads, k_heads, v_heads, w_out, offsets, valid)


def solution(mesh):
    spread = P(("slides", "seq"), "sub")
    return jax.shard_map(
        functools.partial(local, mesh.shape["seq"], mesh.shape["sub"]),
        mesh=mesh,
        in_specs=(spread, spread, spread, P(), P(), P("slides")),
        out_specs=spread,
        check_vma=False,
    )
```

```python
import functools

import jax
import jax.numpy as jnp
from jax import lax
from jax.experimental import pallas as pl
from jax.experimental.pallas import tpu as pltpu
from jax.sharding import PartitionSpec as P

HS = 48
GROUP = 4
R1 = 4
R2 = 16
LANES = 128
HALF = 64
MASKED = -1e30
MESH = pl.DeviceIdType.MESH
EXP_SCALE = HS ** (-0.5) * 1.4426950408889634


def pick(masks, parts):
    out = parts[-1]
    for mask, part in zip(masks[:-1], parts[:-1]):
        out = jnp.where(mask, part, out)
    return out


def kernel(
    n_seq, n_sub, heads,
    q_ref, k_ref, v_ref, w_ref, off_ref, valid_ref, o_ref,
    qp, kx, vx, qm, qw, wide, mid, wk, wv, mk, mv,
    st_m, st_l, st_a, xg, wl, wr, so,
    wide_send, wide_recv, mid_send, mid_recv, x_send, x_recv,
):
    rows = q_ref.shape[1]
    cols = heads * HS
    phase = rows // R1
    strip = rows // R2
    subs = R2 // R1
    half_rows = phase // 2
    seq = lax.axis_index("seq")
    sub = lax.axis_index("sub")
    pos = lax.rem(seq, GROUP)
    group0 = seq - pos
    limit = valid_ref[0]
    has_left = pos > 0
    has_right = pos < GROUP - 1
    bits = [1 << b for b in reversed(range(n_sub.bit_length() - 1))]

    barrier = pltpu.get_barrier_semaphore()
    for step in range(1, n_seq):
        pl.semaphore_signal(
            barrier, inc=1, device_id={"seq": lax.rem(seq + step, n_seq)}, device_id_type=MESH
        )
    for bit in bits:
        pl.semaphore_signal(barrier, inc=1, device_id={"sub": sub ^ bit}, device_id_type=MESH)

    lane = lax.broadcasted_iota(jnp.int32, (1, LANES), 1)
    low = lane < HALF

    def off_lanes(which, first_head, base, tile):
        at = lane + tile * LANES - base
        out = jnp.zeros((1, LANES), jnp.int32)
        for h in range(heads):
            here = ((at >= h * HS) & (at < (h + 1) * HS)) | (at == cols + h)
            out = jnp.where(here, off_ref[which, first_head + h], out)
        return out

    def head_mask(h, base, tiles=2):
        at = lax.broadcasted_iota(jnp.int32, (1, tiles * LANES), 1) - base
        here = (at >= h * HS) & (at < (h + 1) * HS)
        if base == 0:
            here = here | (at == cols + h)
        return here

    mine = sub * heads
    left_off = [[off_lanes(b, mine, 0, t) for t in range(2)] for b in range(2)]
    right_off = [[off_lanes(b, mine, HALF, t) for t in range(2)] for b in range(2)]
    kv_off = [
        [left_off[b][0], jnp.where(low, left_off[b][1], right_off[b][0]), right_off[b][1]]
        for b in range(2)
    ]

    square = R2 * R2
    at_row = lax.broadcasted_iota(jnp.int32, (square, square), 0)
    at_tok = lax.broadcasted_iota(jnp.int32, (square, square), 1)
    one_hot = jnp.where(at_tok == at_row % R2 * R2 + at_row // R2, 1.0, 0.0).astype(jnp.bfloat16)
    contract_last = (((1,), (1,)), ((), ()))
    contract_first = (((0,), (0,)), ((), ()))

    row64 = lax.broadcasted_iota(jnp.int32, (strip, LANES), 0) * R2
    row16 = lax.broadcasted_iota(jnp.int32, (R2, LANES), 0) * R2
    block0 = seq * rows
    with jax.named_scope("load"):
        for blk in range(rows // square):
            toks = pl.ds(blk * square, square)
            kv_t = jnp.concatenate([k_ref[:, toks], v_ref[:, toks]], axis=0)
            q_t = jnp.concatenate([q_ref[:, toks], jnp.ones((HALF, square), jnp.bfloat16)], axis=0)
            kv = lax.dot_general(one_hot, kv_t, contract_last, preferred_element_type=jnp.float32)
            qs = lax.dot_general(one_hot, q_t, contract_last, preferred_element_type=jnp.float32)
            wide_kv = [None] * 3
            wide_q = [None] * 2
            for a in range(subs):
                mid_kv = [None] * 3
                mid_q = [None] * 2
                for m in range(R1):
                    j = a * R1 + m
                    to = pl.ds(m * phase + a * strip + blk * R2, R2)
                    kv_j, q_j = kv[j * R2:(j + 1) * R2], qs[j * R2:(j + 1) * R2]
                    tiles = [kv_j[:, i * LANES:(i + 1) * LANES] for i in range(3)]
                    q_tiles = [q_j[:, i * LANES:(i + 1) * LANES] for i in range(2)]
                    dead = jnp.where(block0 + blk * square + row16 + j < limit, 0.0, MASKED)
                    qp[to, :] = q_j.astype(jnp.bfloat16)
                    kx[to, :LANES] = tiles[0].astype(jnp.bfloat16)
                    kx[to, LANES:] = jnp.where(low, tiles[1], dead).astype(jnp.bfloat16)
                    vx[to, :LANES] = jnp.where(low, 1.0, tiles[1]).astype(jnp.bfloat16)
                    vx[to, LANES:] = tiles[2].astype(jnp.bfloat16)
                    for i, tile in enumerate(tiles):
                        mid_kv[i] = tile if m == 0 else jnp.where(kv_off[0][i] == m, tile, mid_kv[i])
                        wide_kv[i] = tile if j == 0 else jnp.where(kv_off[1][i] == j, tile, wide_kv[i])
                    for i, tile in enumerate(q_tiles):
                        mid_q[i] = tile if m == 0 else jnp.where(left_off[0][i] == m, tile, mid_q[i])
                        wide_q[i] = tile if j == 0 else jnp.where(left_off[1][i] == j, tile, wide_q[i])
                to = pl.ds((a % 2) * strip + blk * R2, R2)
                for i in range(3):
                    mid[pos, a // 2, to, i * LANES:(i + 1) * LANES] = mid_kv[i].astype(jnp.bfloat16)
                to = pl.ds(a * strip + blk * R2, R2)
                for i in range(2):
                    qm[to, i * LANES:(i + 1) * LANES] = mid_q[i].astype(jnp.bfloat16)
            to = pl.ds(blk * R2, R2)
            for i in range(3):
                wide[seq, to, i * LANES:(i + 1) * LANES] = wide_kv[i].astype(jnp.bfloat16)
            for i in range(2):
                qw[to, i * LANES:(i + 1) * LANES] = wide_q[i].astype(jnp.bfloat16)

    with jax.named_scope("barrier"):
        pl.semaphore_wait(barrier, n_seq - 1 + len(bits))

    def wide_copy(origin, step):
        return pltpu.make_async_remote_copy(
            src_ref=wide.at[origin], dst_ref=wide.at[origin],
            send_sem=wide_send.at[step], recv_sem=wide_recv.at[step],
            device_id={"seq": lax.rem(seq + step, n_seq)}, device_id_type=MESH,
        )

    for step in range(1, n_seq):
        wide_copy(seq, step).start()

    def mid_copy(origin, chunk, rightward):
        way = 0 if rightward else 1
        target = seq + 1 if rightward else seq - 1
        return pltpu.make_async_remote_copy(
            src_ref=mid.at[origin, chunk], dst_ref=mid.at[origin, chunk],
            send_sem=mid_send.at[way, origin, chunk], recv_sem=mid_recv.at[origin, chunk],
            device_id={"seq": target}, device_id_type=MESH,
        )

    for chunk in range(2):
        @pl.when(has_right)
        def _():
            mid_copy(pos, chunk, True).start()

        @pl.when(has_left)
        def _():
            mid_copy(pos, chunk, False).start()

    def relay(dist, chunk):
        @pl.when(pos - dist >= 0)
        def _():
            mid_copy(pos - dist, chunk, True).wait_recv()

            @pl.when(has_right)
            def _():
                mid_copy(pos - dist, chunk, True).start()

        @pl.when(pos + dist < GROUP)
        def _():
            mid_copy(pos + dist, chunk, False).wait_recv()

            @pl.when(has_left)
            def _():
                mid_copy(pos + dist, chunk, False).start()

    with jax.named_scope("weights"):
        for d in range(n_sub):
            wl[d, pl.ds(cols, HALF), :] = jnp.zeros((HALF, cols), jnp.bfloat16)
            wr[d, pl.ds(0, HALF), :] = jnp.zeros((HALF, cols), jnp.bfloat16)
        for s in range(n_sub):
            @pl.when(sub == s)
            def _():
                for d in range(n_sub):
                    part = w_ref[d * cols:(d + 1) * cols, s * cols:(s + 1) * cols]
                    wl[d, pl.ds(0, cols), :] = part
                    wr[d, pl.ds(HALF, cols), :] = part

    def attend(q_blk, keys, values, h, before=None):
        masked_q = jnp.where(head_mask(h, 0), q_blk.astype(jnp.float32), 0.0).astype(jnp.bfloat16)
        scores = lax.dot_general(masked_q, keys, contract_last, preferred_element_type=jnp.float32)
        peak = jnp.max(scores, axis=1, keepdims=True)
        if before is not None:
            peak = jnp.maximum(peak, before)
        probs = jnp.exp2((scores - peak) * EXP_SCALE).astype(jnp.bfloat16)
        return peak, jnp.dot(probs, values, preferred_element_type=jnp.float32)

    def near_step(m, carry):
        at = pl.ds(pl.multiple_of(m * phase, phase), phase)
        q_blk = qp[at, :]
        acc = top = mass = None
        for h in range(heads):
            peak, out = attend(q_blk, kx[...], vx[...], h)
            here = head_mask(h, HALF)
            total = out[:, 0:1]
            shape = out.shape
            if h == 0:
                acc, top, mass = out, jnp.broadcast_to(peak, shape), jnp.broadcast_to(total, shape)
            else:
                acc = jnp.where(here, out, acc)
                top = jnp.where(here, peak, top)
                mass = jnp.where(here, total, mass)
        st_a[at, :] = acc
        st_m[at, :] = top
        st_l[at, :] = mass

        @pl.when(m == 2)
        def _():
            relay(1, 0)

        return carry

    with jax.named_scope("near"):
        lax.fori_loop(0, R1, near_step, 0)
    relay(1, 1)

    def merge(q_blk, keys, values, top, mass, acc):
        for h in range(heads):
            here = head_mask(h, HALF)
            before = jnp.max(jnp.where(here, top, -3e38), axis=1, keepdims=True)
            peak, out = attend(q_blk, keys, values, h, before)
            fade = jnp.exp2((before - peak) * EXP_SCALE)
            total = out[:, 0:1]
            acc = jnp.where(here, acc * fade + out, acc)
            mass = jnp.where(here, mass * fade + total, mass)
            top = jnp.where(here, peak, top)
        return top, mass, acc

    r_off = [jnp.concatenate(right_off[b], axis=1) for b in range(2)]
    wide_lane_off = left_off[1][1]
    with jax.named_scope("wide_wait"):
        for step in range(1, n_seq):
            wide_copy(lax.rem(seq + n_seq - step, n_seq), step).wait_recv()
    for o in range(n_seq):
        at = pl.ds(o * strip, strip)
        tile1 = wide[o, :, LANES:2 * LANES].astype(jnp.float32)
        dead = jnp.where(o * rows + row64 + wide_lane_off < limit, 0.0, MASKED)
        wk[at, :LANES] = wide[o, :, :LANES]
        wk[at, LANES:] = jnp.where(low, tile1, dead).astype(jnp.bfloat16)
        wv[at, :LANES] = jnp.where(low, 1.0, tile1).astype(jnp.bfloat16)
        wv[at, LANES:] = wide[o, :, 2 * LANES:]

    def strip_at(j):
        return pl.ds((j % R1) * phase + (j // R1) * strip, strip)

    with jax.named_scope("wide_merge"):
        wide_masks = [r_off[1] == j for j in range(R2)]
        state = [pick(wide_masks, [ref[strip_at(j), :] for j in range(R2)]) for ref in (st_m, st_l, st_a)]
        state = merge(qw[...], wk[...], wv[...], *state)
        for ref, new in zip((st_m, st_l, st_a), state):
            for j in range(R2):
                ref[strip_at(j), :] = jnp.where(wide_masks[j], new, ref[strip_at(j), :])

    def pack(slab, value):
        top_half, bot = value[:half_rows], value[half_rows:]
        moved = pltpu.roll(top_half, LANES + HALF, 1)
        xg[sub, slab, :, :LANES] = moved[:, :LANES].astype(jnp.bfloat16)
        xg[sub, slab, :, LANES:2 * LANES] = jnp.where(
            low, moved[:, LANES:], bot[:, :LANES]
        ).astype(jnp.bfloat16)
        xg[sub, slab, :, 2 * LANES:] = bot[:, LANES:].astype(jnp.bfloat16)

    def x_copy(at_bit, held, slab):
        bit = bits[at_bit]
        block = sub ^ held
        return pltpu.make_async_remote_copy(
            src_ref=xg.at[block, slab], dst_ref=xg.at[block, slab],
            send_sem=x_send.at[at_bit, held, slab], recv_sem=x_recv.at[held ^ bit, slab],
            device_id={"sub": sub ^ bit}, device_id_type=MESH,
        )

    def x_plan():
        held, plan = [0], []
        for at_bit, bit in enumerate(bits):
            plan += [(at_bit, x) for x in held]
            held = held + [x ^ bit for x in held]
        return plan

    def x_start(slab):
        for at_bit, x in x_plan():
            if x == 0:
                x_copy(at_bit, x, slab).start()

    def x_recv_wait(block, slab):
        pltpu.make_async_remote_copy(
            src_ref=xg.at[sub ^ block, slab], dst_ref=xg.at[sub ^ block, slab],
            send_sem=x_send.at[0, 0, slab], recv_sem=x_recv.at[block, slab],
            device_id={"sub": sub ^ block}, device_id_type=MESH,
        ).wait_recv()

    def x_forward(slab):
        waited = set()
        for at_bit, x in x_plan():
            if x:
                if x not in waited:
                    waited.add(x)
                    x_recv_wait(x, slab)
                x_copy(at_bit, x, slab).start()
        return waited

    def x_finish(slab, waited):
        for x in range(1, n_sub):
            if x not in waited:
                x_recv_wait(x, slab)

    mid_masks = [r_off[0] == m for m in range(R1)]
    with jax.named_scope("slabs"):
        for slab in range(1, R1):
            parts = []
            for m in range(R1):
                at = pl.ds(m * phase, phase)
                parts.append(st_a[at, :] / st_l[at, :])
            pack(slab, pick([mid_masks[(m - slab) % R1] for m in range(R1)], parts))
            x_start(slab)

    with jax.named_scope("relays"):
        for chunk in range(2):
            relay(2, chunk)
        for chunk in range(2):
            relay(3, chunk)

    mid_lane_off = left_off[0][1]
    pair_row = lax.broadcasted_iota(jnp.int32, (half_rows, LANES), 0)
    pair_row = (pair_row % strip) * R2 + (pair_row // strip) * R1
    with jax.named_scope("mid_merge"):
        for o in range(GROUP):
            for chunk in range(2):
                at = pl.ds(o * phase + chunk * half_rows, half_rows)
                tile1 = mid[o, chunk, :, LANES:2 * LANES].astype(jnp.float32)
                place = (group0 + o) * rows + pair_row + (chunk * 2 * R1 + mid_lane_off)
                dead = jnp.where(place < limit, 0.0, MASKED)
                mk[at, :LANES] = mid[o, chunk, :, :LANES]
                mk[at, LANES:] = jnp.where(low, tile1, dead).astype(jnp.bfloat16)
                mv[at, :LANES] = jnp.where(low, 1.0, tile1).astype(jnp.bfloat16)
                mv[at, LANES:] = mid[o, chunk, :, 2 * LANES:]
        state = [
            pick(mid_masks, [ref[pl.ds(m * phase, phase), :] for m in range(R1)])
            for ref in (st_m, st_l, st_a)
        ]
        state = merge(qm[...], mk[...], mv[...], *state)
        pack(0, state[2] / state[1])
        x_start(0)

    with jax.named_scope("x_wait"):
        done = {}
        for slab in (1, 2, 3, 0):
            done[slab] = x_forward(slab)
        for slab in (1, 2, 3, 0):
            x_finish(slab, done[slab])

    with jax.named_scope("project"):
        outs = [[None, None] for _ in range(R1)]
        for d in range(n_sub):
            offs = [
                jnp.concatenate([off_lanes(0, d * heads, base, t) for t in range(2)], axis=1)
                for base in (0, HALF)
            ]
            for half in range(2):
                take = slice(half * LANES, half * LANES + 2 * LANES)
                slabs = [xg[d, i, :, take].astype(jnp.float32) for i in range(R1)]
                weights = (wl, wr)[half][d]
                for m in range(R1):
                    masks = [offs[half] == (m - i) % R1 for i in range(R1)]
                    term = jnp.dot(
                        pick(masks, slabs).astype(jnp.bfloat16), weights,
                        preferred_element_type=jnp.float32,
                    )
                    outs[m][half] = term if d == 0 else outs[m][half] + term
        for m in range(R1):
            for half in range(2):
                so[pl.ds(m * phase + half * half_rows, half_rows), :] = outs[m][half].astype(jnp.bfloat16)
        for blk in range(rows // square):
            picked = jnp.concatenate(
                [
                    so[pl.ds((j % R1) * phase + (j // R1) * strip + blk * R2, R2), :]
                    for j in range(R2)
                ],
                axis=0,
            )
            res = lax.dot_general(picked, one_hot, contract_first, preferred_element_type=jnp.float32)
            place = block0 + blk * square + lax.broadcasted_iota(jnp.int32, (1, square), 1)
            o_ref[:, pl.ds(blk * square, square)] = jnp.where(place < limit, res, 0.0).astype(jnp.bfloat16)

    with jax.named_scope("drain"):
        for step in range(1, n_seq):
            wide_copy(seq, step).wait_send()
        for chunk in range(2):
            for o in range(GROUP):
                @pl.when(has_right & (pos >= o))
                def _():
                    mid_copy(o, chunk, True).wait_send()

                @pl.when(has_left & (pos <= o))
                def _():
                    mid_copy(o, chunk, False).wait_send()
        for slab in range(R1):
            for at_bit, x in x_plan():
                x_copy(at_bit, x, slab).wait_send()


def local(n_seq, n_sub, q_heads, k_heads, v_heads, w_out, offsets, valid):
    rows, cols = q_heads.shape
    heads = cols // HS
    phase, strip = rows // R1, rows // R2
    bf, f32 = jnp.bfloat16, jnp.float32
    n_bits = n_sub.bit_length() - 1
    assert cols == LANES + HALF and n_sub == 1 << n_bits
    vmem = pl.BlockSpec(memory_space=pltpu.VMEM)
    smem = pl.BlockSpec(memory_space=pltpu.SMEM)
    wide_all = n_seq * strip
    return pl.pallas_call(
        functools.partial(kernel, n_seq, n_sub, heads),
        out_shape=jax.ShapeDtypeStruct((cols, rows), bf),
        in_specs=[vmem] * 4 + [smem] * 2,
        out_specs=vmem,
        scratch_shapes=[
            pltpu.VMEM((rows, 2 * LANES), bf),
            pltpu.VMEM((rows, 2 * LANES), bf),
            pltpu.VMEM((rows, 2 * LANES), bf),
            pltpu.VMEM((phase, 2 * LANES), bf),
            pltpu.VMEM((strip, 2 * LANES), bf),
            pltpu.VMEM((n_seq, strip, 3 * LANES), bf),
            pltpu.VMEM((GROUP, 2, phase // 2, 3 * LANES), bf),
            pltpu.VMEM((wide_all, 2 * LANES), bf),
            pltpu.VMEM((wide_all, 2 * LANES), bf),
            pltpu.VMEM((GROUP * phase, 2 * LANES), bf),
            pltpu.VMEM((GROUP * phase, 2 * LANES), bf),
            pltpu.VMEM((rows, 2 * LANES), f32),
            pltpu.VMEM((rows, 2 * LANES), f32),
            pltpu.VMEM((rows, 2 * LANES), f32),
            pltpu.VMEM((n_sub, R1, phase // 2, 3 * LANES), bf),
            pltpu.VMEM((n_sub, 2 * LANES, cols), bf),
            pltpu.VMEM((n_sub, 2 * LANES, cols), bf),
            pltpu.VMEM((rows, cols), bf),
            pltpu.SemaphoreType.DMA((n_seq,)),
            pltpu.SemaphoreType.DMA((n_seq,)),
            pltpu.SemaphoreType.DMA((2, GROUP, 2)),
            pltpu.SemaphoreType.DMA((GROUP, 2)),
            pltpu.SemaphoreType.DMA((n_bits, n_sub, R1)),
            pltpu.SemaphoreType.DMA((n_sub, R1)),
        ],
        compiler_params=pltpu.CompilerParams(
            collective_id=0, has_side_effects=True, vmem_limit_bytes=56 * 1024 * 1024
        ),
    )(q_heads.T, k_heads.T, v_heads.T, w_out, offsets, valid).T


def solution(mesh):
    spread = P(("slides", "seq"), "sub")
    return jax.shard_map(
        functools.partial(local, mesh.shape["seq"], mesh.shape["sub"]),
        mesh=mesh,
        in_specs=(spread, spread, spread, P(), P(), P("slides")),
        out_specs=spread,
        check_vma=False,
    )
```

```python
import functools

import jax
import jax.numpy as jnp
from jax import lax
from jax.experimental import pallas as pl
from jax.experimental.pallas import tpu as pltpu
from jax.sharding import PartitionSpec as P

HS = 48
GROUP = 4
R1 = 4
R2 = 16
LANES = 128
HALF = 64
MASKED = -1e30
MESH = pl.DeviceIdType.MESH
EXP_SCALE = HS ** (-0.5) * 1.4426950408889634


def pick(masks, parts):
    out = parts[-1]
    for mask, part in zip(masks[:-1], parts[:-1]):
        out = jnp.where(mask, part, out)
    return out


def kernel(
    n_seq, n_sub, heads,
    q_hbm, k_hbm, v_hbm, w_hbm, off_ref, valid_ref, o_ref,
    q_ref, k_ref, v_ref, w_ref,
    qp, kx, vx, qw, wide, mid, wk, wv, mk, mv,
    st_m, st_l, st_a, xg, xw, wl, wr, so, at_x,
    wide_send, wide_recv, mid_send, mid_recv, x_send, x_recv, in_sem,
):
    rows = q_ref.shape[1]
    cols = heads * HS
    phase = rows // R1
    strip = rows // R2
    subs = R2 // R1
    half_rows = phase // 2
    seq = lax.axis_index("seq")
    sub = lax.axis_index("sub")
    pos = lax.rem(seq, GROUP)
    group0 = seq - pos
    limit = valid_ref[0]
    has_left = pos > 0
    has_right = pos < GROUP - 1
    bits = [1 << b for b in reversed(range(n_sub.bit_length() - 1))]

    fetches = [
        pltpu.make_async_copy(src, dst, in_sem.at[i])
        for i, (src, dst) in enumerate(
            ((k_hbm, k_ref), (v_hbm, v_ref), (q_hbm, q_ref), (w_hbm, w_ref))
        )
    ]
    for fetch in fetches:
        fetch.start()
    barrier = pltpu.get_barrier_semaphore()
    for step in (1, n_seq - 1):
        pl.semaphore_signal(
            barrier, inc=1, device_id={"seq": lax.rem(seq + step, n_seq)}, device_id_type=MESH
        )
    for bit in bits:
        pl.semaphore_signal(barrier, inc=1, device_id={"sub": sub ^ bit}, device_id_type=MESH)

    lane = lax.broadcasted_iota(jnp.int32, (1, LANES), 1)
    low = lane < HALF

    def off_lanes(which, first_head, base, tile):
        at = lane + tile * LANES - base
        out = jnp.zeros((1, LANES), jnp.int32)
        for h in range(heads):
            here = ((at >= h * HS) & (at < (h + 1) * HS)) | (at == cols + h)
            out = jnp.where(here, off_ref[which, first_head + h], out)
        return out

    def head_mask(h, base, tiles=2):
        at = lax.broadcasted_iota(jnp.int32, (1, tiles * LANES), 1) - base
        here = (at >= h * HS) & (at < (h + 1) * HS)
        if base == 0:
            here = here | (at == cols + h)
        return here

    mine = sub * heads
    left_off = [[off_lanes(b, mine, 0, t) for t in range(2)] for b in range(2)]
    right_off = [[off_lanes(b, mine, HALF, t) for t in range(2)] for b in range(2)]
    kv_off = [
        [left_off[b][0], jnp.where(low, left_off[b][1], right_off[b][0]), right_off[b][1]]
        for b in range(2)
    ]

    square = R2 * R2
    at_row = lax.broadcasted_iota(jnp.int32, (square, square), 0)
    at_tok = lax.broadcasted_iota(jnp.int32, (square, square), 1)
    one_hot = jnp.where(at_tok == at_row % R2 * R2 + at_row // R2, 1.0, 0.0).astype(jnp.bfloat16)
    contract_last = (((1,), (1,)), ((), ()))
    contract_first = (((0,), (0,)), ((), ()))

    turned = [[lax.rem(off + s, R1) for off in left_off[0]] for s in range(R1)]
    row64 = lax.broadcasted_iota(jnp.int32, (strip, LANES), 0) * R2
    row16 = lax.broadcasted_iota(jnp.int32, (R2, LANES), 0) * R2
    block0 = seq * rows
    with jax.named_scope("load"):
        for fetch in fetches[:3]:
            fetch.wait()
        for blk in range(rows // square):
            toks = pl.ds(blk * square, square)
            kv_t = jnp.concatenate([k_ref[:, toks], v_ref[:, toks]], axis=0)
            q_t = jnp.concatenate([q_ref[:, toks], jnp.ones((HALF, square), jnp.bfloat16)], axis=0)
            kv = lax.dot_general(one_hot, kv_t, contract_last, preferred_element_type=jnp.float32)
            qs = lax.dot_general(one_hot, q_t, contract_last, preferred_element_type=jnp.float32)
            wide_kv = [None] * 3
            wide_q = [None] * 2
            for a in range(subs):
                mid_kv = [None] * 3
                slab_q = [[None] * 2 for _ in range(R1)]
                for m in range(R1):
                    j = a * R1 + m
                    to = pl.ds(m * phase + a * strip + blk * R2, R2)
                    kv_j, q_j = kv[j * R2:(j + 1) * R2], qs[j * R2:(j + 1) * R2]
                    tiles = [kv_j[:, i * LANES:(i + 1) * LANES] for i in range(3)]
                    q_tiles = [q_j[:, i * LANES:(i + 1) * LANES] for i in range(2)]
                    dead = jnp.where(block0 + blk * square + row16 + j < limit, 0.0, MASKED)
                    kx[to, :LANES] = tiles[0].astype(jnp.bfloat16)
                    kx[to, LANES:] = jnp.where(low, tiles[1], dead).astype(jnp.bfloat16)
                    vx[to, :LANES] = jnp.where(low, 1.0, tiles[1]).astype(jnp.bfloat16)
                    vx[to, LANES:] = tiles[2].astype(jnp.bfloat16)
                    for i, tile in enumerate(tiles):
                        mid_kv[i] = tile if m == 0 else jnp.where(kv_off[0][i] == m, tile, mid_kv[i])
                        wide_kv[i] = tile if j == 0 else jnp.where(kv_off[1][i] == j, tile, wide_kv[i])
                    for i, tile in enumerate(q_tiles):
                        for s in range(R1):
                            here = turned[s][i] == m
                            slab_q[s][i] = tile if m == 0 else jnp.where(here, tile, slab_q[s][i])
                        wide_q[i] = tile if j == 0 else jnp.where(left_off[1][i] == j, tile, wide_q[i])
                to = pl.ds((a % 2) * strip + blk * R2, R2)
                for i in range(3):
                    mid[pos, a // 2, to, i * LANES:(i + 1) * LANES] = mid_kv[i].astype(jnp.bfloat16)
                for s in range(R1):
                    to = pl.ds(s * phase + a * strip + blk * R2, R2)
                    for i in range(2):
                        qp[to, i * LANES:(i + 1) * LANES] = slab_q[s][i].astype(jnp.bfloat16)
            to = pl.ds(blk * R2, R2)
            for i in range(3):
                wide[seq, to, i * LANES:(i + 1) * LANES] = wide_kv[i].astype(jnp.bfloat16)
            for i in range(2):
                qw[to, i * LANES:(i + 1) * LANES] = wide_q[i].astype(jnp.bfloat16)

    with jax.named_scope("barrier"):
        pl.semaphore_wait(barrier, 2 + len(bits))

    def wide_copy(origin, rightward):
        target = seq + 1 if rightward else seq - 1
        return pltpu.make_async_remote_copy(
            src_ref=wide.at[origin], dst_ref=wide.at[origin],
            send_sem=wide_send.at[0 if rightward else 1, origin], recv_sem=wide_recv.at[origin],
            device_id={"seq": target}, device_id_type=MESH,
        )

    @pl.when(seq < n_seq - 1)
    def _():
        wide_copy(seq, True).start()

    @pl.when(seq > 0)
    def _():
        wide_copy(seq, False).start()

    def wide_relay(dist):
        @pl.when(seq - dist >= 0)
        def _():
            wide_copy(seq - dist, True).wait_recv()

            @pl.when(seq < n_seq - 1)
            def _():
                wide_copy(seq - dist, True).start()

        @pl.when(seq + dist < n_seq)
        def _():
            wide_copy(seq + dist, False).wait_recv()

            @pl.when(seq > 0)
            def _():
                wide_copy(seq + dist, False).start()

    def mid_copy(origin, chunk, rightward):
        way = 0 if rightward else 1
        target = seq + 1 if rightward else seq - 1
        return pltpu.make_async_remote_copy(
            src_ref=mid.at[origin, chunk], dst_ref=mid.at[origin, chunk],
            send_sem=mid_send.at[way, origin, chunk], recv_sem=mid_recv.at[origin, chunk],
            device_id={"seq": target}, device_id_type=MESH,
        )

    for chunk in range(2):
        @pl.when(has_right)
        def _():
            mid_copy(pos, chunk, True).start()

        @pl.when(has_left)
        def _():
            mid_copy(pos, chunk, False).start()

    def relay(dist, chunk):
        @pl.when(pos - dist >= 0)
        def _():
            mid_copy(pos - dist, chunk, True).wait_recv()

            @pl.when(has_right)
            def _():
                mid_copy(pos - dist, chunk, True).start()

        @pl.when(pos + dist < GROUP)
        def _():
            mid_copy(pos + dist, chunk, False).wait_recv()

            @pl.when(has_left)
            def _():
                mid_copy(pos + dist, chunk, False).start()

    with jax.named_scope("weights"):
        fetches[3].wait()
        for d in range(n_sub):
            wl[pl.ds(d * 2 * LANES + cols, HALF), :] = jnp.zeros((HALF, cols), jnp.bfloat16)
            wr[pl.ds(d * 2 * LANES, HALF), :] = jnp.zeros((HALF, cols), jnp.bfloat16)
        for s in range(n_sub):
            @pl.when(sub == s)
            def _():
                for d in range(n_sub):
                    part = w_ref[d * cols:(d + 1) * cols, s * cols:(s + 1) * cols]
                    wl[pl.ds(d * 2 * LANES, cols), :] = part
                    wr[pl.ds(d * 2 * LANES + HALF, cols), :] = part

    def attend(q_blk, keys, values, h, before=None):
        masked_q = jnp.where(head_mask(h, 0), q_blk.astype(jnp.float32), 0.0).astype(jnp.bfloat16)
        scores = lax.dot_general(masked_q, keys, contract_last, preferred_element_type=jnp.float32)
        peak = jnp.max(scores, axis=1, keepdims=True)
        if before is not None:
            peak = jnp.maximum(peak, before)
        probs = jnp.exp2((scores - peak) * EXP_SCALE).astype(jnp.bfloat16)
        return peak, jnp.dot(probs, values, preferred_element_type=jnp.float32)

    def pack(slab, value):
        dst = xw.at[sub] if slab is None else xg.at[sub, slab]
        top_half, bot = value[:value.shape[0] // 2], value[value.shape[0] // 2:]
        moved = pltpu.roll(top_half, LANES + HALF, 1)
        dst[:, :LANES] = moved[:, :LANES].astype(jnp.bfloat16)
        dst[:, LANES:2 * LANES] = jnp.where(
            low, moved[:, LANES:], bot[:, :LANES]
        ).astype(jnp.bfloat16)
        dst[:, 2 * LANES:] = bot[:, LANES:].astype(jnp.bfloat16)

    def x_ref(block, slab):
        return xw.at[block] if isinstance(slab, int) and slab == R1 else xg.at[block, slab]

    def x_copy(at_bit, held, slab):
        bit = bits[at_bit]
        ref = x_ref(sub ^ held, slab)
        return pltpu.make_async_remote_copy(
            src_ref=ref, dst_ref=ref,
            send_sem=x_send.at[at_bit, held, slab], recv_sem=x_recv.at[held ^ bit, slab],
            device_id={"sub": sub ^ bit}, device_id_type=MESH,
        )

    def x_plan():
        held, plan = [0], []
        for at_bit, bit in enumerate(bits):
            plan += [(at_bit, x) for x in held]
            held = held + [x ^ bit for x in held]
        return plan

    def x_start(slab):
        for at_bit, x in x_plan():
            if x == 0:
                x_copy(at_bit, x, slab).start()

    def x_recv_wait(block, slab):
        ref = x_ref(sub ^ block, slab)
        pltpu.make_async_remote_copy(
            src_ref=ref, dst_ref=ref,
            send_sem=x_send.at[0, 0, slab], recv_sem=x_recv.at[block, slab],
            device_id={"sub": sub ^ block}, device_id_type=MESH,
        ).wait_recv()

    def x_forward(slab):
        waited = set()
        for at_bit, x in x_plan():
            if x:
                if x not in waited:
                    waited.add(x)
                    x_recv_wait(x, slab)
                x_copy(at_bit, x, slab).start()
        return waited

    def x_finish(slab, waited):
        for x in range(1, n_sub):
            if x not in waited:
                x_recv_wait(x, slab)

    def near_step(it, carry):
        slab = lax.rem(it + 1, R1)
        at = pl.ds(pl.multiple_of(slab * phase, phase), phase)
        q_blk = qp[at, :]
        acc = top = mass = None
        for h in range(heads):
            peak, out = attend(q_blk, kx[...], vx[...], h)
            here = head_mask(h, HALF)
            total = out[:, 0:1]
            shape = out.shape
            if h == 0:
                acc, top, mass = out, jnp.broadcast_to(peak, shape), jnp.broadcast_to(total, shape)
            else:
                acc = jnp.where(here, out, acc)
                top = jnp.where(here, peak, top)
                mass = jnp.where(here, total, mass)
        st_a[at, :] = acc
        st_m[at, :] = top
        st_l[at, :] = mass

        @pl.when(it < R1 - 1)
        def _():
            pack(slab, acc / mass)
            x_start(slab)

        @pl.when(it == 1)
        def _():
            wide_relay(1)
            relay(1, 0)

        @pl.when(it == 2)
        def _():
            wide_relay(2)
            relay(1, 1)
            x_forward(1)

        @pl.when(it == 3)
        def _():
            for dist in range(3, n_seq):
                wide_relay(dist)
            relay(2, 0)
            x_forward(2)

        return carry

    with jax.named_scope("near"):
        lax.fori_loop(0, R1, near_step, 0)

    def merge(q_blk, keys, values, top, mass, acc):
        for h in range(heads):
            here = head_mask(h, HALF)
            before = jnp.max(jnp.where(here, top, -3e38), axis=1, keepdims=True)
            peak, out = attend(q_blk, keys, values, h, before)
            fade = jnp.exp2((before - peak) * EXP_SCALE)
            total = out[:, 0:1]
            acc = jnp.where(here, acc * fade + out, acc)
            mass = jnp.where(here, mass * fade + total, mass)
            top = jnp.where(here, peak, top)
        return top, mass, acc

    mid_lane_off = left_off[0][1]
    pair_row = lax.broadcasted_iota(jnp.int32, (half_rows, LANES), 0)
    pair_row = (pair_row % strip) * R2 + (pair_row // strip) * R1
    pair = GROUP // 2
    own_pair = lax.div(pos, pair)

    def mid_merge(which):
        for o in range(pair):
            origin = which * pair + o
            for chunk in range(2):
                to = pl.ds(o * phase + chunk * half_rows, half_rows)
                tile1 = mid[origin, chunk, :, LANES:2 * LANES].astype(jnp.float32)
                place = (group0 + origin) * rows + pair_row + (chunk * 2 * R1 + mid_lane_off)
                dead = jnp.where(place < limit, 0.0, MASKED)
                mk[to, :LANES] = mid[origin, chunk, :, :LANES]
                mk[to, LANES:] = jnp.where(low, tile1, dead).astype(jnp.bfloat16)
                mv[to, :LANES] = jnp.where(low, 1.0, tile1).astype(jnp.bfloat16)
                mv[to, LANES:] = mid[origin, chunk, :, 2 * LANES:]
        at = pl.ds(0, phase)
        return merge(qp[at, :], mk[...], mv[...], st_m[at, :], st_l[at, :], st_a[at, :])

    with jax.named_scope("mid_merge_own"):
        for ref, new in zip((st_m, st_l, st_a), mid_merge(own_pair)):
            ref[pl.ds(0, phase), :] = new
        relay(2, 1)
        x_forward(3)

    r_off = [jnp.concatenate(right_off[b], axis=1) for b in range(2)]
    wide_lane_off = left_off[1][1]
    for o in range(n_seq):
        at = pl.ds(o * strip, strip)
        tile1 = wide[o, :, LANES:2 * LANES].astype(jnp.float32)
        dead = jnp.where(o * rows + row64 + wide_lane_off < limit, 0.0, MASKED)
        wk[at, :LANES] = wide[o, :, :LANES]
        wk[at, LANES:] = jnp.where(low, tile1, dead).astype(jnp.bfloat16)
        wv[at, :LANES] = jnp.where(low, 1.0, tile1).astype(jnp.bfloat16)
        wv[at, LANES:] = wide[o, :, 2 * LANES:]

    with jax.named_scope("wide_merge"):
        slab_of = lax.rem(r_off[1] + R1 - r_off[0], R1)
        part_of = lax.div(r_off[1], R1)
        strip_of = slab_of * subs + part_of
        wide_masks = [strip_of == j for j in range(R2)]
        state = [
            pick(wide_masks, [ref[pl.ds(j * strip, strip), :] for j in range(R2)])
            for ref in (st_m, st_l, st_a)
        ]
        state = merge(qw[...], wk[...], wv[...], *state)
        for ref, new in zip((st_m, st_l, st_a), state):
            for j in range(subs):
                at = pl.ds(j * strip, strip)
                ref[at, :] = jnp.where(wide_masks[j], new, ref[at, :])
        wide_out = state[2] / state[1]
    with jax.named_scope("relays"):
        for chunk in range(2):
            relay(3, chunk)

    with jax.named_scope("mid_merge"):
        state = mid_merge(1 - own_pair)
        mid_out = state[2] / state[1]
        pack(0, mid_out)
        x_start(0)
        parts = [mid_out[a * strip:(a + 1) * strip] for a in range(subs)]
        shared = pick([part_of == a for a in range(subs)], parts)
        pack(None, jnp.where(slab_of == 0, shared, wide_out))
        x_start(R1)
    with jax.named_scope("x_wait"):
        relayed = {x for at_bit, x in x_plan() if x}
        done = {slab: relayed for slab in range(1, R1)}
        for slab in (0, R1):
            done[slab] = x_forward(slab)
        for slab in (1, 2, 3, 0, R1):
            x_finish(slab, done[slab])

    with jax.named_scope("project"):
        for d in range(n_sub):
            offs, wide_offs = [
                [
                    jnp.concatenate([off_lanes(b, d * heads, base, t) for t in range(2)], axis=1)
                    for base in (0, HALF)
                ]
                for b in range(2)
            ]
            first = xw[d, :, :2 * LANES].astype(jnp.float32)
            second = xw[d, :, LANES:].astype(jnp.float32)
            wide_rows = [
                jnp.concatenate([first, pltpu.roll(second, LANES + HALF, 1)], axis=0),
                jnp.concatenate([pltpu.roll(first, HALF, 1), second], axis=0),
            ]
            for half in range(2):
                take = slice(half * LANES, half * LANES + 2 * LANES)
                slabs = [xg[d, i, :, take].astype(jnp.float32) for i in range(R1)]
                spare = wide_rows[half]
                for m in range(R1):
                    masks = [offs[half] == (m - i) % R1 for i in range(R1)]
                    rows_m = pick(masks, slabs)
                    rows_m = jnp.concatenate(
                        [
                            jnp.where(
                                wide_offs[half] == (half * 2 + i) * R1 + m, spare,
                                rows_m[i * strip:(i + 1) * strip],
                            )
                            for i in range(2)
                        ],
                        axis=0,
                    )
                    at_x[half, pl.ds(m * half_rows, half_rows), pl.ds(d * 2 * LANES, 2 * LANES)] = (
                        rows_m.astype(jnp.bfloat16)
                    )
        for half in range(2):
            out = jnp.dot(at_x[half], (wl, wr)[half][...], preferred_element_type=jnp.float32)
            out = out.astype(jnp.bfloat16)
            for m in range(R1):
                to = pl.ds(m * phase + half * half_rows, half_rows)
                so[to, :] = out[m * half_rows:(m + 1) * half_rows]
        for blk in range(rows // square):
            picked = jnp.concatenate(
                [
                    so[pl.ds((j % R1) * phase + (j // R1) * strip + blk * R2, R2), :]
                    for j in range(R2)
                ],
                axis=0,
            )
            res = lax.dot_general(picked, one_hot, contract_first, preferred_element_type=jnp.float32)
            place = block0 + blk * square + lax.broadcasted_iota(jnp.int32, (1, square), 1)
            o_ref[:, pl.ds(blk * square, square)] = jnp.where(place < limit, res, 0.0).astype(jnp.bfloat16)

    with jax.named_scope("drain"):
        for o in range(n_seq):
            @pl.when((seq < n_seq - 1) & (seq >= o))
            def _():
                wide_copy(o, True).wait_send()

            @pl.when((seq > 0) & (seq <= o))
            def _():
                wide_copy(o, False).wait_send()
        for chunk in range(2):
            for o in range(GROUP):
                @pl.when(has_right & (pos >= o))
                def _():
                    mid_copy(o, chunk, True).wait_send()

                @pl.when(has_left & (pos <= o))
                def _():
                    mid_copy(o, chunk, False).wait_send()
        for slab in range(R1 + 1):
            for at_bit, x in x_plan():
                x_copy(at_bit, x, slab).wait_send()


def local(n_seq, n_sub, q_heads, k_heads, v_heads, w_out, offsets, valid):
    rows, cols = q_heads.shape
    heads = cols // HS
    phase, strip = rows // R1, rows // R2
    bf, f32 = jnp.bfloat16, jnp.float32
    n_bits = n_sub.bit_length() - 1
    assert cols == LANES + HALF and n_sub == 1 << n_bits
    vmem = pl.BlockSpec(memory_space=pltpu.VMEM)
    smem = pl.BlockSpec(memory_space=pltpu.SMEM)
    wide_all = n_seq * strip
    return pl.pallas_call(
        functools.partial(kernel, n_seq, n_sub, heads),
        out_shape=jax.ShapeDtypeStruct((cols, rows), bf),
        in_specs=[pl.BlockSpec(memory_space=pl.ANY)] * 4 + [smem] * 2,
        out_specs=vmem,
        scratch_shapes=[
            pltpu.VMEM((cols, rows), bf),
            pltpu.VMEM((cols, rows), bf),
            pltpu.VMEM((cols, rows), bf),
            pltpu.VMEM(w_out.shape, bf),
            pltpu.VMEM((rows, 2 * LANES), bf),
            pltpu.VMEM((rows, 2 * LANES), bf),
            pltpu.VMEM((rows, 2 * LANES), bf),
            pltpu.VMEM((strip, 2 * LANES), bf),
            pltpu.VMEM((n_seq, strip, 3 * LANES), bf),
            pltpu.VMEM((GROUP, 2, phase // 2, 3 * LANES), bf),
            pltpu.VMEM((wide_all, 2 * LANES), bf),
            pltpu.VMEM((wide_all, 2 * LANES), bf),
            pltpu.VMEM((GROUP // 2 * phase, 2 * LANES), bf),
            pltpu.VMEM((GROUP // 2 * phase, 2 * LANES), bf),
            pltpu.VMEM((rows, 2 * LANES), f32),
            pltpu.VMEM((rows, 2 * LANES), f32),
            pltpu.VMEM((rows, 2 * LANES), f32),
            pltpu.VMEM((n_sub, R1, phase // 2, 3 * LANES), bf),
            pltpu.VMEM((n_sub, strip // 2, 3 * LANES), bf),
            pltpu.VMEM((n_sub * 2 * LANES, cols), bf),
            pltpu.VMEM((n_sub * 2 * LANES, cols), bf),
            pltpu.VMEM((rows, cols), bf),
            pltpu.VMEM((2, rows // 2, n_sub * 2 * LANES), bf),
            pltpu.SemaphoreType.DMA((2, n_seq)),
            pltpu.SemaphoreType.DMA((n_seq,)),
            pltpu.SemaphoreType.DMA((2, GROUP, 2)),
            pltpu.SemaphoreType.DMA((GROUP, 2)),
            pltpu.SemaphoreType.DMA((n_bits, n_sub, R1 + 1)),
            pltpu.SemaphoreType.DMA((n_sub, R1 + 1)),
            pltpu.SemaphoreType.DMA((4,)),
        ],
        compiler_params=pltpu.CompilerParams(
            collective_id=0, has_side_effects=True, vmem_limit_bytes=56 * 1024 * 1024
        ),
    )(q_heads.T, k_heads.T, v_heads.T, w_out, offsets, valid).T


def solution(mesh):
    spread = P(("slides", "seq"), "sub")
    return jax.shard_map(
        functools.partial(local, mesh.shape["seq"], mesh.shape["sub"]),
        mesh=mesh,
        in_specs=(spread, spread, spread, P(), P(), P("slides")),
        out_specs=spread,
        check_vma=False,
    )
```

```python
import functools

import jax
import jax.numpy as jnp
from jax import lax
from jax.experimental import pallas as pl
from jax.experimental.pallas import tpu as pltpu
from jax.sharding import PartitionSpec as P

HS = 48
GROUP = 4
R1 = 4
R2 = 16
LANES = 128
HALF = 64
MASKED = -1e30
MESH = pl.DeviceIdType.MESH
EXP_SCALE = HS ** (-0.5) * 1.4426950408889634


def pick(masks, parts):
    out = parts[-1]
    for mask, part in zip(masks[:-1], parts[:-1]):
        out = jnp.where(mask, part, out)
    return out


def kernel(
    n_seq, n_sub, heads,
    q_hbm, k_hbm, v_hbm, w_hbm, off_ref, valid_ref, o_ref,
    q_ref, k_ref, v_ref, w_ref,
    qp, kx, vx, qw, wide, mid, wk, wv, mk, mv,
    st_m, st_l, st_a, xg, xw, wl, wr, so, at_x,
    wide_send, wide_recv, mid_send, mid_recv, x_send, x_recv, in_sem,
):
    rows = q_ref.shape[1]
    cols = heads * HS
    phase = rows // R1
    strip = rows // R2
    subs = R2 // R1
    half_rows = phase // 2
    seq = lax.axis_index("seq")
    sub = lax.axis_index("sub")
    pos = lax.rem(seq, GROUP)
    group0 = seq - pos
    limit = valid_ref[0]
    has_left = pos > 0
    has_right = pos < GROUP - 1
    bits = [1 << b for b in reversed(range(n_sub.bit_length() - 1))]

    fetches = [
        pltpu.make_async_copy(src, dst, in_sem.at[i])
        for i, (src, dst) in enumerate(
            ((k_hbm, k_ref), (v_hbm, v_ref), (q_hbm, q_ref), (w_hbm, w_ref))
        )
    ]
    for fetch in fetches:
        fetch.start()
    barrier = pltpu.get_barrier_semaphore()
    for step in (1, n_seq - 1):
        pl.semaphore_signal(
            barrier, inc=1, device_id={"seq": lax.rem(seq + step, n_seq)}, device_id_type=MESH
        )
    for bit in bits:
        pl.semaphore_signal(barrier, inc=1, device_id={"sub": sub ^ bit}, device_id_type=MESH)

    lane = lax.broadcasted_iota(jnp.int32, (1, LANES), 1)
    low = lane < HALF

    def off_lanes(which, first_head, base, tile):
        at = lane + tile * LANES - base
        out = jnp.zeros((1, LANES), jnp.int32)
        for h in range(heads):
            here = ((at >= h * HS) & (at < (h + 1) * HS)) | (at == cols + h)
            out = jnp.where(here, off_ref[which, first_head + h], out)
        return out

    def head_mask(h, base, tiles=2):
        at = lax.broadcasted_iota(jnp.int32, (1, tiles * LANES), 1) - base
        here = (at >= h * HS) & (at < (h + 1) * HS)
        if base == 0:
            here = here | (at == cols + h)
        return here

    mine = sub * heads
    left_off = [[off_lanes(b, mine, 0, t) for t in range(2)] for b in range(2)]
    right_off = [[off_lanes(b, mine, HALF, t) for t in range(2)] for b in range(2)]
    kv_off = [
        [left_off[b][0], jnp.where(low, left_off[b][1], right_off[b][0]), right_off[b][1]]
        for b in range(2)
    ]

    square = R2 * R2
    at_row = lax.broadcasted_iota(jnp.int32, (square, square), 0)
    at_tok = lax.broadcasted_iota(jnp.int32, (square, square), 1)
    one_hot = jnp.where(at_tok == at_row % R2 * R2 + at_row // R2, 1.0, 0.0).astype(jnp.bfloat16)
    contract_last = (((1,), (1,)), ((), ()))
    contract_first = (((0,), (0,)), ((), ()))

    turned = [[lax.rem(off + s, R1) for off in left_off[0]] for s in range(R1)]
    row64 = lax.broadcasted_iota(jnp.int32, (strip, LANES), 0) * R2
    row16 = lax.broadcasted_iota(jnp.int32, (R2, LANES), 0) * R2
    block0 = seq * rows
    with jax.named_scope("load"):
        for fetch in fetches[:3]:
            fetch.wait()
        for blk in range(rows // square):
            toks = pl.ds(blk * square, square)
            kv_t = jnp.concatenate([k_ref[:, toks], v_ref[:, toks]], axis=0)
            q_t = jnp.concatenate([q_ref[:, toks], jnp.ones((HALF, square), jnp.bfloat16)], axis=0)
            kv = lax.dot_general(one_hot, kv_t, contract_last, preferred_element_type=jnp.float32)
            qs = lax.dot_general(one_hot, q_t, contract_last, preferred_element_type=jnp.float32)
            wide_kv = [None] * 3
            wide_q = [None] * 2
            for a in range(subs):
                mid_kv = [None] * 3
                slab_q = [[None] * 2 for _ in range(R1)]
                for m in range(R1):
                    j = a * R1 + m
                    to = pl.ds(m * phase + a * strip + blk * R2, R2)
                    kv_j, q_j = kv[j * R2:(j + 1) * R2], qs[j * R2:(j + 1) * R2]
                    tiles = [kv_j[:, i * LANES:(i + 1) * LANES] for i in range(3)]
                    q_tiles = [q_j[:, i * LANES:(i + 1) * LANES] for i in range(2)]
                    dead = jnp.where(block0 + blk * square + row16 + j < limit, 0.0, MASKED)
                    kx[to, :LANES] = tiles[0].astype(jnp.bfloat16)
                    kx[to, LANES:] = jnp.where(low, tiles[1], dead).astype(jnp.bfloat16)
                    vx[to, :LANES] = jnp.where(low, 1.0, tiles[1]).astype(jnp.bfloat16)
                    vx[to, LANES:] = tiles[2].astype(jnp.bfloat16)
                    for i, tile in enumerate(tiles):
                        mid_kv[i] = tile if m == 0 else jnp.where(kv_off[0][i] == m, tile, mid_kv[i])
                        wide_kv[i] = tile if j == 0 else jnp.where(kv_off[1][i] == j, tile, wide_kv[i])
                    for i, tile in enumerate(q_tiles):
                        for s in range(R1):
                            here = turned[s][i] == m
                            slab_q[s][i] = tile if m == 0 else jnp.where(here, tile, slab_q[s][i])
                        wide_q[i] = tile if j == 0 else jnp.where(left_off[1][i] == j, tile, wide_q[i])
                to = pl.ds((a % 2) * strip + blk * R2, R2)
                for i in range(3):
                    mid[pos, a // 2, to, i * LANES:(i + 1) * LANES] = mid_kv[i].astype(jnp.bfloat16)
                for s in range(R1):
                    to = pl.ds(s * phase + a * strip + blk * R2, R2)
                    for i in range(2):
                        qp[to, i * LANES:(i + 1) * LANES] = slab_q[s][i].astype(jnp.bfloat16)
            to = pl.ds(blk * R2, R2)
            for i in range(3):
                wide[seq, to, i * LANES:(i + 1) * LANES] = wide_kv[i].astype(jnp.bfloat16)
            for i in range(2):
                qw[to, i * LANES:(i + 1) * LANES] = wide_q[i].astype(jnp.bfloat16)

    with jax.named_scope("barrier"):
        pl.semaphore_wait(barrier, 2 + len(bits))

    def wide_copy(origin, rightward):
        target = seq + 1 if rightward else seq - 1
        return pltpu.make_async_remote_copy(
            src_ref=wide.at[origin], dst_ref=wide.at[origin],
            send_sem=wide_send.at[0 if rightward else 1, origin], recv_sem=wide_recv.at[origin],
            device_id={"seq": target}, device_id_type=MESH,
        )

    @pl.when(seq < n_seq - 1)
    def _():
        wide_copy(seq, True).start()

    @pl.when(seq > 0)
    def _():
        wide_copy(seq, False).start()

    def wide_relay(dist):
        @pl.when(seq - dist >= 0)
        def _():
            wide_copy(seq - dist, True).wait_recv()

            @pl.when(seq < n_seq - 1)
            def _():
                wide_copy(seq - dist, True).start()

        @pl.when(seq + dist < n_seq)
        def _():
            wide_copy(seq + dist, False).wait_recv()

            @pl.when(seq > 0)
            def _():
                wide_copy(seq + dist, False).start()

    def mid_copy(origin, chunk, rightward):
        way = 0 if rightward else 1
        target = seq + 1 if rightward else seq - 1
        return pltpu.make_async_remote_copy(
            src_ref=mid.at[origin, chunk], dst_ref=mid.at[origin, chunk],
            send_sem=mid_send.at[way, origin, chunk], recv_sem=mid_recv.at[origin, chunk],
            device_id={"seq": target}, device_id_type=MESH,
        )

    for chunk in range(2):
        @pl.when(has_right)
        def _():
            mid_copy(pos, chunk, True).start()

        @pl.when(has_left)
        def _():
            mid_copy(pos, chunk, False).start()

    def relay(dist, chunk):
        @pl.when(pos - dist >= 0)
        def _():
            mid_copy(pos - dist, chunk, True).wait_recv()

            @pl.when(has_right)
            def _():
                mid_copy(pos - dist, chunk, True).start()

        @pl.when(pos + dist < GROUP)
        def _():
            mid_copy(pos + dist, chunk, False).wait_recv()

            @pl.when(has_left)
            def _():
                mid_copy(pos + dist, chunk, False).start()

    with jax.named_scope("weights"):
        fetches[3].wait()
        for d in range(n_sub):
            wl[pl.ds(d * 2 * LANES + cols, HALF), :] = jnp.zeros((HALF, cols), jnp.bfloat16)
            wr[pl.ds(d * 2 * LANES, HALF), :] = jnp.zeros((HALF, cols), jnp.bfloat16)
        for s in range(n_sub):
            @pl.when(sub == s)
            def _():
                for d in range(n_sub):
                    part = w_ref[d * cols:(d + 1) * cols, s * cols:(s + 1) * cols]
                    wl[pl.ds(d * 2 * LANES, cols), :] = part
                    wr[pl.ds(d * 2 * LANES + HALF, cols), :] = part

    def attend(q_blk, keys, values, h, before=None):
        masked_q = jnp.where(head_mask(h, 0), q_blk.astype(jnp.float32), 0.0).astype(jnp.bfloat16)
        scores = lax.dot_general(masked_q, keys, contract_last, preferred_element_type=jnp.float32)
        peak = jnp.max(scores, axis=1, keepdims=True)
        if before is not None:
            peak = jnp.maximum(peak, before)
        probs = jnp.exp2((scores - peak) * EXP_SCALE).astype(jnp.bfloat16)
        return peak, jnp.dot(probs, values, preferred_element_type=jnp.float32)

    def pack(slab, value):
        dst = xw.at[sub] if slab is None else xg.at[sub, slab]
        top_half, bot = value[:value.shape[0] // 2], value[value.shape[0] // 2:]
        moved = pltpu.roll(top_half, LANES + HALF, 1)
        dst[:, :LANES] = moved[:, :LANES].astype(jnp.bfloat16)
        dst[:, LANES:2 * LANES] = jnp.where(
            low, moved[:, LANES:], bot[:, :LANES]
        ).astype(jnp.bfloat16)
        dst[:, 2 * LANES:] = bot[:, LANES:].astype(jnp.bfloat16)

    def x_ref(block, slab):
        return xw.at[block] if isinstance(slab, int) and slab == R1 else xg.at[block, slab]

    def x_copy(at_bit, held, slab):
        bit = bits[at_bit]
        ref = x_ref(sub ^ held, slab)
        return pltpu.make_async_remote_copy(
            src_ref=ref, dst_ref=ref,
            send_sem=x_send.at[at_bit, held, slab], recv_sem=x_recv.at[held ^ bit, slab],
            device_id={"sub": sub ^ bit}, device_id_type=MESH,
        )

    def x_plan():
        held, plan = [0], []
        for at_bit, bit in enumerate(bits):
            plan += [(at_bit, x) for x in held]
            held = held + [x ^ bit for x in held]
        return plan

    def x_start(slab):
        for at_bit, x in x_plan():
            if x == 0:
                x_copy(at_bit, x, slab).start()

    def x_recv_wait(block, slab):
        ref = x_ref(sub ^ block, slab)
        pltpu.make_async_remote_copy(
            src_ref=ref, dst_ref=ref,
            send_sem=x_send.at[0, 0, slab], recv_sem=x_recv.at[block, slab],
            device_id={"sub": sub ^ block}, device_id_type=MESH,
        ).wait_recv()

    def x_forward(slab):
        waited = set()
        for at_bit, x in x_plan():
            if x:
                if x not in waited:
                    waited.add(x)
                    x_recv_wait(x, slab)
                x_copy(at_bit, x, slab).start()
        return waited

    def x_finish(slab, waited):
        for x in range(1, n_sub):
            if x not in waited:
                x_recv_wait(x, slab)

    def near_step(it, carry):
        slab = lax.rem(it + 1, R1)
        at = pl.ds(pl.multiple_of(slab * phase, phase), phase)
        q_blk = qp[at, :]
        acc = top = mass = None
        for h in range(heads):
            peak, out = attend(q_blk, kx[...], vx[...], h)
            here = head_mask(h, HALF)
            total = out[:, 0:1]
            shape = out.shape
            if h == 0:
                acc, top, mass = out, jnp.broadcast_to(peak, shape), jnp.broadcast_to(total, shape)
            else:
                acc = jnp.where(here, out, acc)
                top = jnp.where(here, peak, top)
                mass = jnp.where(here, total, mass)
        st_a[at, :] = acc
        st_m[at, :] = top
        st_l[at, :] = mass

        @pl.when(it < R1 - 1)
        def _():
            pack(slab, acc / mass)
            x_start(slab)

        @pl.when(it == 1)
        def _():
            wide_relay(1)
            relay(1, 0)

        @pl.when(it == 2)
        def _():
            wide_relay(2)
            relay(1, 1)
            x_forward(1)

        @pl.when(it == 3)
        def _():
            for dist in range(3, n_seq):
                wide_relay(dist)
            relay(2, 0)
            x_forward(2)

        return carry

    with jax.named_scope("near"):
        lax.fori_loop(0, R1, near_step, 0)

    def merge(q_blk, keys, values, top, mass, acc):
        for h in range(heads):
            here = head_mask(h, HALF)
            before = jnp.max(jnp.where(here, top, -3e38), axis=1, keepdims=True)
            peak, out = attend(q_blk, keys, values, h, before)
            fade = jnp.exp2((before - peak) * EXP_SCALE)
            total = out[:, 0:1]
            acc = jnp.where(here, acc * fade + out, acc)
            mass = jnp.where(here, mass * fade + total, mass)
            top = jnp.where(here, peak, top)
        return top, mass, acc

    mid_lane_off = left_off[0][1]
    pair_row = lax.broadcasted_iota(jnp.int32, (half_rows, LANES), 0)
    pair_row = (pair_row % strip) * R2 + (pair_row // strip) * R1
    pair = GROUP // 2
    own_pair = lax.div(pos, pair)

    def mid_merge(which):
        for o in range(pair):
            origin = which * pair + o
            for chunk in range(2):
                to = pl.ds(o * phase + chunk * half_rows, half_rows)
                tile1 = mid[origin, chunk, :, LANES:2 * LANES].astype(jnp.float32)
                place = (group0 + origin) * rows + pair_row + (chunk * 2 * R1 + mid_lane_off)
                dead = jnp.where(place < limit, 0.0, MASKED)
                mk[to, :LANES] = mid[origin, chunk, :, :LANES]
                mk[to, LANES:] = jnp.where(low, tile1, dead).astype(jnp.bfloat16)
                mv[to, :LANES] = jnp.where(low, 1.0, tile1).astype(jnp.bfloat16)
                mv[to, LANES:] = mid[origin, chunk, :, 2 * LANES:]
        at = pl.ds(0, phase)
        return merge(qp[at, :], mk[...], mv[...], st_m[at, :], st_l[at, :], st_a[at, :])

    with jax.named_scope("mid_merge_own"):
        for ref, new in zip((st_m, st_l, st_a), mid_merge(own_pair)):
            ref[pl.ds(0, phase), :] = new
        relay(2, 1)
        x_forward(3)

    r_off = [jnp.concatenate(right_off[b], axis=1) for b in range(2)]
    wide_lane_off = left_off[1][1]
    for o in range(n_seq):
        at = pl.ds(o * strip, strip)
        tile1 = wide[o, :, LANES:2 * LANES].astype(jnp.float32)
        dead = jnp.where(o * rows + row64 + wide_lane_off < limit, 0.0, MASKED)
        wk[at, :LANES] = wide[o, :, :LANES]
        wk[at, LANES:] = jnp.where(low, tile1, dead).astype(jnp.bfloat16)
        wv[at, :LANES] = jnp.where(low, 1.0, tile1).astype(jnp.bfloat16)
        wv[at, LANES:] = wide[o, :, 2 * LANES:]

    with jax.named_scope("wide_merge"):
        slab_of = lax.rem(r_off[1] + R1 - r_off[0], R1)
        part_of = lax.div(r_off[1], R1)
        strip_of = slab_of * subs + part_of
        wide_masks = [strip_of == j for j in range(R2)]
        state = [
            pick(wide_masks, [ref[pl.ds(j * strip, strip), :] for j in range(R2)])
            for ref in (st_m, st_l, st_a)
        ]
        state = merge(qw[...], wk[...], wv[...], *state)
        for ref, new in zip((st_m, st_l, st_a), state):
            for j in range(subs):
                at = pl.ds(j * strip, strip)
                ref[at, :] = jnp.where(wide_masks[j], new, ref[at, :])
        wide_out = state[2] / state[1]
    with jax.named_scope("relays"):
        for chunk in range(2):
            relay(3, chunk)

    with jax.named_scope("mid_merge"):
        state = mid_merge(1 - own_pair)
        mid_out = state[2] / state[1]
        pack(0, mid_out)
        x_start(0)
        parts = [mid_out[a * strip:(a + 1) * strip] for a in range(subs)]
        shared = pick([part_of == a for a in range(subs)], parts)
        pack(None, jnp.where(slab_of == 0, shared, wide_out))
        x_start(R1)
    with jax.named_scope("x_wait"):
        relayed = {x for at_bit, x in x_plan() if x}
        done = {slab: relayed for slab in range(1, R1)}
        for slab in (0, R1):
            done[slab] = x_forward(slab)
        for slab in (1, 2, 3, 0, R1):
            x_finish(slab, done[slab])

    with jax.named_scope("project"):
        for d in range(n_sub):
            offs, wide_offs = [
                [
                    jnp.concatenate([off_lanes(b, d * heads, base, t) for t in range(2)], axis=1)
                    for base in (0, HALF)
                ]
                for b in range(2)
            ]
            first = xw[d, :, :2 * LANES].astype(jnp.float32)
            second = xw[d, :, LANES:].astype(jnp.float32)
            wide_rows = [
                jnp.concatenate([first, pltpu.roll(second, LANES + HALF, 1)], axis=0),
                jnp.concatenate([pltpu.roll(first, HALF, 1), second], axis=0),
            ]
            for half in range(2):
                take = slice(half * LANES, half * LANES + 2 * LANES)
                slabs = [xg[d, i, :, take].astype(jnp.float32) for i in range(R1)]
                spare = wide_rows[half]
                for m in range(R1):
                    masks = [offs[half] == (m - i) % R1 for i in range(R1)]
                    rows_m = pick(masks, slabs)
                    rows_m = jnp.concatenate(
                        [
                            jnp.where(
                                wide_offs[half] == (half * 2 + i) * R1 + m, spare,
                                rows_m[i * strip:(i + 1) * strip],
                            )
                            for i in range(2)
                        ],
                        axis=0,
                    )
                    at_x[half, pl.ds(m * half_rows, half_rows), pl.ds(d * 2 * LANES, 2 * LANES)] = (
                        rows_m.astype(jnp.bfloat16)
                    )
        for half in range(2):
            out = jnp.dot(at_x[half], (wl, wr)[half][...], preferred_element_type=jnp.float32)
            out = out.astype(jnp.bfloat16)
            for m in range(R1):
                to = pl.ds(m * phase + half * half_rows, half_rows)
                so[to, :] = out[m * half_rows:(m + 1) * half_rows]
        for blk in range(rows // square):
            picked = jnp.concatenate(
                [
                    so[pl.ds((j % R1) * phase + (j // R1) * strip + blk * R2, R2), :]
                    for j in range(R2)
                ],
                axis=0,
            )
            res = lax.dot_general(picked, one_hot, contract_first, preferred_element_type=jnp.float32)
            o_ref[:, pl.ds(blk * square, square)] = res.astype(jnp.bfloat16)

    with jax.named_scope("drain"):
        for o in range(n_seq):
            @pl.when((seq < n_seq - 1) & (seq >= o))
            def _():
                wide_copy(o, True).wait_send()

            @pl.when((seq > 0) & (seq <= o))
            def _():
                wide_copy(o, False).wait_send()
        for chunk in range(2):
            for o in range(GROUP):
                @pl.when(has_right & (pos >= o))
                def _():
                    mid_copy(o, chunk, True).wait_send()

                @pl.when(has_left & (pos <= o))
                def _():
                    mid_copy(o, chunk, False).wait_send()
        for slab in range(R1 + 1):
            for at_bit, x in x_plan():
                x_copy(at_bit, x, slab).wait_send()


def local(n_seq, n_sub, q_heads, k_heads, v_heads, w_out, offsets, valid):
    rows, cols = q_heads.shape
    heads = cols // HS
    phase, strip = rows // R1, rows // R2
    bf, f32 = jnp.bfloat16, jnp.float32
    n_bits = n_sub.bit_length() - 1
    assert cols == LANES + HALF and n_sub == 1 << n_bits
    vmem = pl.BlockSpec(memory_space=pltpu.VMEM)
    smem = pl.BlockSpec(memory_space=pltpu.SMEM)
    wide_all = n_seq * strip
    out = pl.pallas_call(
        functools.partial(kernel, n_seq, n_sub, heads),
        out_shape=jax.ShapeDtypeStruct((cols, rows), bf),
        in_specs=[pl.BlockSpec(memory_space=pl.ANY)] * 4 + [smem] * 2,
        out_specs=vmem,
        scratch_shapes=[
            pltpu.VMEM((cols, rows), bf),
            pltpu.VMEM((cols, rows), bf),
            pltpu.VMEM((cols, rows), bf),
            pltpu.VMEM(w_out.shape, bf),
            pltpu.VMEM((rows, 2 * LANES), bf),
            pltpu.VMEM((rows, 2 * LANES), bf),
            pltpu.VMEM((rows, 2 * LANES), bf),
            pltpu.VMEM((strip, 2 * LANES), bf),
            pltpu.VMEM((n_seq, strip, 3 * LANES), bf),
            pltpu.VMEM((GROUP, 2, phase // 2, 3 * LANES), bf),
            pltpu.VMEM((wide_all, 2 * LANES), bf),
            pltpu.VMEM((wide_all, 2 * LANES), bf),
            pltpu.VMEM((GROUP // 2 * phase, 2 * LANES), bf),
            pltpu.VMEM((GROUP // 2 * phase, 2 * LANES), bf),
            pltpu.VMEM((rows, 2 * LANES), f32),
            pltpu.VMEM((rows, 2 * LANES), f32),
            pltpu.VMEM((rows, 2 * LANES), f32),
            pltpu.VMEM((n_sub, R1, phase // 2, 3 * LANES), bf),
            pltpu.VMEM((n_sub, strip // 2, 3 * LANES), bf),
            pltpu.VMEM((n_sub * 2 * LANES, cols), bf),
            pltpu.VMEM((n_sub * 2 * LANES, cols), bf),
            pltpu.VMEM((rows, cols), bf),
            pltpu.VMEM((2, rows // 2, n_sub * 2 * LANES), bf),
            pltpu.SemaphoreType.DMA((2, n_seq)),
            pltpu.SemaphoreType.DMA((n_seq,)),
            pltpu.SemaphoreType.DMA((2, GROUP, 2)),
            pltpu.SemaphoreType.DMA((GROUP, 2)),
            pltpu.SemaphoreType.DMA((n_bits, n_sub, R1 + 1)),
            pltpu.SemaphoreType.DMA((n_sub, R1 + 1)),
            pltpu.SemaphoreType.DMA((4,)),
        ],
        compiler_params=pltpu.CompilerParams(
            collective_id=0, has_side_effects=True, vmem_limit_bytes=32 * 1024 * 1024
        ),
    )(q_heads.T, k_heads.T, v_heads.T, w_out, offsets, valid)
    place = lax.axis_index("seq") * rows + lax.broadcasted_iota(jnp.int32, (1, rows), 1)
    return jnp.where(place < valid[0], out, jnp.zeros((), bf)).T


def solution(mesh):
    spread = P(("slides", "seq"), "sub")
    return jax.shard_map(
        functools.partial(local, mesh.shape["seq"], mesh.shape["sub"]),
        mesh=mesh,
        in_specs=(spread, spread, spread, P(), P(), P("slides")),
        out_specs=spread,
        check_vma=False,
    )
```
